1024 devices in a mesh: grp: 8 (over z_lo), cp: 128 (over y, x, z_hi, core).
Axes of the slice: x: 4, y: 4, z: 32 (z_hi: 4, z_lo: 8; z = z_hi * 8 + z_lo), core: 2. Of those that a mesh axis runs over, the one named last changes fastest.
Arguments:
- query_states: bfloat16 [1024, 256, 1024], P(('grp', 'cp')), may hold values from -130 to 130
- key_states: bfloat16 [1024, 256, 128], P(('grp', 'cp')), may hold values from -8 to 8
- value_states: bfloat16 [1024, 256, 128], P(('grp', 'cp')), may hold values from -6 to 6
- grad_output: bfloat16 [1024, 256, 1024], P(('grp', 'cp')), may hold values from -6 to 6
- pair_kinds: int32 [512, 7], replicated, may hold values from 0 to 3, as said below
- row_start: int32 [65536], replicated, may hold values from 0 to 65534, as said below
Outputs:
- attn_out: bfloat16 [1024, 256, 1024], P(('grp', 'cp'))
- grad_query: bfloat16 [1024, 256, 1024], P(('grp', 'cp'))
- grad_key: bfloat16 [1024, 256, 128], P(('grp', 'cp'))
- grad_value: bfloat16 [1024, 256, 128], P(('grp', 'cp'))
The draws below stay inside these ranges and needn't reach their ends.
Inputs may be any that keep to these rules, and one draw needn't show every extreme that they name: `pair_kinds`: kinds are 0 to 3 as in the reference program; column 0 is 1 or 2; [b, d] is 3 wherever b - d < 0. row_start[t] lies between max(t - 768, 0) and max(t - 1, 0).
All inputs are finite; a program needn't handle non-finite values.
Results may differ from the reference program's by a relative error of at most 0.035.
Values may be sent and summed in bfloat16 or wider, within the bound.
A program may use at most 32 MiB of HBM per device.

```python
from functools import partial
import jax
import jax.numpy as jnp
from jax import lax

KVH = 4
HD = 128
BLK = 128
REACH = 6
GQ = 8
OWNERS = 256
ROWS_DEV = 256
NB = 512
TOKENS = 65536


def shared_fields(key):
    folded = jax.random.fold_in(key, 11)
    draw_one, draw_two = jax.random.split(folded, 2)
    queries = jnp.clip(jax.random.normal(draw_one, (OWNERS * KVH, ROWS_DEV, GQ, HD), jnp.float32), -6.0, 6.0)
    states = jnp.clip(jax.random.normal(draw_two, (OWNERS * KVH, ROWS_DEV, HD), jnp.float32), -6.0, 6.0)
    return (queries, states)


def draw_query_states(key, part):
    queries, states = shared_fields(key)
    return queries.reshape(OWNERS * KVH, ROWS_DEV, GQ * HD).astype(jnp.bfloat16)


def draw_key_states(key, part):
    queries, states = shared_fields(key)
    return states.astype(jnp.bfloat16)


def draw_pair_kinds(key, part):
    folded = jax.random.fold_in(key, 23)
    draw_one, draw_two, draw_three, draw_four = jax.random.split(folded, 4)
    density = jax.random.randint(draw_one, (NB, 1), 0, REACH + 1)
    ranking = jax.random.randint(draw_two, (NB, REACH), 0, REACH)
    full_or_bounded = jax.random.randint(draw_three, (NB, REACH), 0, 2) * 2
    distant = jnp.where(ranking < density, full_or_bounded, 3)
    block_ids = jnp.arange(NB, dtype=jnp.int32)[:, None]
    distance = jnp.arange(1, REACH + 1, dtype=jnp.int32)[None, :]
    distant = jnp.where(block_ids - distance >= 0, distant, 3)
    diagonal = 1 + jax.random.randint(draw_four, (NB, 1), 0, 2)
    return jnp.concatenate([diagonal, distant], axis=1).astype(jnp.int32)


def draw_row_start(key, part):
    reach_rows = jax.random.randint(jax.random.fold_in(key, 31), (TOKENS,), 1, REACH * BLK + 1)
    return jnp.maximum(jnp.arange(TOKENS, dtype=jnp.int32) - reach_rows, 0).astype(jnp.int32)


def levels(stream_key, dims, cuts, least, high):
    level = 1.0
    for axis_at, parts in cuts:
        heights = jax.random.uniform(jax.random.fold_in(jax.random.fold_in(stream_key, 6), axis_at), (parts,), jnp.float32, least / len(cuts), high / len(cuts))
        level = level * jnp.repeat(jnp.exp(heights), dims[axis_at] // parts).reshape((-1,) + (1,) * (len(dims) - 1 - axis_at))
    return level


def normal_values(stream_key, extent, scale, bound, shards=(), kind=jnp.bfloat16):
    result = jax.random.normal(stream_key, extent, jnp.float32) * scale
    if len(shards) > 0:
        result = levels(stream_key, extent, shards, -0.22, 0.18) * result
    return jnp.clip(result, min=-bound, max=bound).astype(kind)


def setup_inputs(seed: int = 0) -> dict:
    streams_of = jax.random.split(jax.random.key(seed), 7)
    query_states = draw_query_states(jax.random.fold_in(streams_of[6], 71), 0)
    key_states = draw_key_states(jax.random.fold_in(streams_of[6], 71), 0)
    value_states = normal_values(streams_of[2], (OWNERS * KVH, ROWS_DEV, HD), 1.0, 6.0, ((0, 1024),))
    grad_output = normal_values(streams_of[3], (OWNERS * KVH, ROWS_DEV, GQ * HD), 1.0, 6.0, ((0, 1024),))
    pair_kinds = draw_pair_kinds(jax.random.fold_in(streams_of[6], 71), 0)
    row_start = draw_row_start(jax.random.fold_in(streams_of[6], 71), 0)
    return {"query_states": query_states, "key_states": key_states, "value_states": value_states, "grad_output": grad_output, "pair_kinds": pair_kinds, "row_start": row_start}


def window_mask(kinds_block, starts_block, row_first):
    window_width = (REACH + 1) * BLK
    query_pos = row_first + jnp.arange(BLK, dtype=jnp.int32)
    key_pos = row_first - REACH * BLK + jnp.arange(window_width, dtype=jnp.int32)
    kind_cols = jnp.repeat(kinds_block[::-1], BLK)
    before = key_pos[None, :] <= query_pos[:, None]
    inside = before & (key_pos[None, :] >= starts_block[:, None])
    return (kind_cols == 0)[None, :] | ((kind_cols == 1)[None, :] & before) | ((kind_cols == 2)[None, :] & inside)


def head_pass(fields, pair_kinds, row_start):
    head_queries, head_keys, head_values, head_grads = fields
    front_pad = REACH * BLK
    window_width = (REACH + 1) * BLK
    score_scale = HD ** -0.5
    padded_keys = jnp.concatenate([jnp.zeros((front_pad, HD), head_keys.dtype), head_keys], axis=0)
    padded_values = jnp.concatenate([jnp.zeros((front_pad, HD), head_values.dtype), head_values], axis=0)

    def advance(state, block_number):
        grad_keys, grad_values = state
        row_first = block_number * BLK
        query_block = lax.dynamic_slice_in_dim(head_queries, row_first, BLK, 0).astype(jnp.float32)
        grad_block = lax.dynamic_slice_in_dim(head_grads, row_first, BLK, 0).astype(jnp.float32)
        key_window = lax.dynamic_slice_in_dim(padded_keys, row_first, window_width, 0).astype(jnp.float32)
        value_window = lax.dynamic_slice_in_dim(padded_values, row_first, window_width, 0).astype(jnp.float32)
        kinds_block = lax.dynamic_slice_in_dim(pair_kinds, block_number, 1, 0)[0]
        starts_block = lax.dynamic_slice_in_dim(row_start, row_first, BLK, 0)
        allowed = window_mask(kinds_block, starts_block, row_first)
        scores = jnp.einsum("qgd,wd->gqw", query_block, key_window) * score_scale
        scores = jnp.where(allowed[None], scores, -jnp.inf)
        row_max = jnp.max(scores, axis=-1, keepdims=True)
        log_total = row_max + jnp.log(jnp.sum(jnp.exp(scores - row_max), axis=-1, keepdims=True))
        prob_full = jnp.exp(scores - log_total)
        prob_half = lax.optimization_barrier(prob_full.astype(jnp.bfloat16)).astype(jnp.float32)
        block_out = jnp.einsum("gqw,wd->qgd", prob_half, value_window).astype(jnp.bfloat16)
        out_wide = lax.optimization_barrier(block_out).astype(jnp.float32)
        row_dot = jnp.sum(grad_block * out_wide, axis=-1).T[:, :, None]
        prob_grad = jnp.einsum("qgd,wd->gqw", grad_block, value_window)
        score_grad = lax.optimization_barrier((prob_full * (prob_grad - row_dot)).astype(jnp.bfloat16)).astype(jnp.float32)
        query_grad = (jnp.einsum("gqw,wd->qgd", score_grad, key_window) * score_scale).astype(jnp.bfloat16)
        key_part = jnp.einsum("gqw,qgd->wd", score_grad, query_block) * score_scale
        value_part = jnp.einsum("gqw,qgd->wd", prob_half, grad_block)
        grad_keys = lax.dynamic_update_slice_in_dim(grad_keys, lax.dynamic_slice_in_dim(grad_keys, row_first, window_width, 0) + key_part, row_first, 0)
        grad_values = lax.dynamic_update_slice_in_dim(grad_values, lax.dynamic_slice_in_dim(grad_values, row_first, window_width, 0) + value_part, row_first, 0)
        return (grad_keys, grad_values), (block_out, query_grad)

    initial = (jnp.zeros((TOKENS + front_pad, HD), jnp.float32), jnp.zeros((TOKENS + front_pad, HD), jnp.float32))
    (grad_keys, grad_values), (block_outs, query_grads) = lax.scan(advance, initial, jnp.arange(TOKENS // BLK, dtype=jnp.int32))
    return (block_outs.reshape(TOKENS, GQ * HD), query_grads.reshape(TOKENS, GQ * HD), grad_keys[front_pad:].astype(jnp.bfloat16), grad_values[front_pad:].astype(jnp.bfloat16))


def by_head(array, trailing):
    return array.reshape((OWNERS, KVH, ROWS_DEV) + trailing).swapaxes(0, 1).reshape((KVH, TOKENS) + trailing)


def to_slots(array):
    return array.reshape(KVH, OWNERS, ROWS_DEV, -1).swapaxes(0, 1).reshape(OWNERS * KVH, ROWS_DEV, -1)


def reference(query_states, key_states, value_states, grad_output, pair_kinds, row_start):
    heads = (by_head(query_states, (GQ, HD)), by_head(key_states, (HD,)), by_head(value_states, (HD,)), by_head(grad_output, (GQ, HD)))
    attn_all, qgrad_all, kgrad_all, vgrad_all = lax.map(partial(head_pass, pair_kinds=pair_kinds, row_start=row_start), heads)
    return (to_slots(attn_all), to_slots(qgrad_all), to_slots(kgrad_all), to_slots(vgrad_all))
```

```python
import jax
import jax.numpy as jnp
from jax import lax
from jax.experimental import pallas as pl
from jax.experimental.pallas import tpu as pltpu
from jax.sharding import PartitionSpec as P

KVH = 4
HD = 128
BLK = 128
REACH = 6
GQ = 8
ROWS = 256
PAIRS = GQ // 2
MESH = pl.DeviceIdType.MESH
FAR = 1 << 30
LOG2E = 1.4426950408889634

BACK3, BACK1, BACK2, OWN = 0, 512, 256, 768


def nt(a, b):
    return lax.dot_general(a, b, (((1,), (1,)), ((), ())), preferred_element_type=jnp.float32)


def nn(a, b):
    return lax.dot_general(a, b, (((1,), (0,)), ((), ())), preferred_element_type=jnp.float32)


def block_row(b, d):
    return (REACH + 1 + b - 1 - d) * BLK


def kernel(
    q_hbm, k_hbm, v_hbm, g_hbm, kinds_hbm, start_hbm,
    out_hbm, gq_hbm, gk_hbm, gv_hbm,
    q_ref, g_ref, keys, vals, keys_t, vals_t, bias, kinds, starts,
    prob, pgrad, prob_half, score_half, top8, dot8, acc_k, acc_v,
    part3, sum1, part2, got3, got1, got2, gotx, out_ref, gq_ref, final,
    local_sem, send_sem, recv_sem,
):
    grp, cp = lax.axis_index("grp"), lax.axis_index("cp")
    linear = grp * 128 + cp
    owner = linear // KVH
    z_hi = lax.rem(cp // 2, 4)
    side = z_hi // 2

    def along(step):
        moved = lax.rem(linear + step + 1024, 1024)
        return moved // 128, lax.rem(moved, 128)

    later, earlier = along(2 * KVH), along(-2 * KVH)
    across = (grp, cp + 4 - 8 * side)

    barrier = pltpu.get_barrier_semaphore()
    for peer in (later, earlier, across):
        pl.semaphore_signal(barrier, inc=1, device_id=peer, device_id_type=MESH)

    tile = pl.multiple_of((owner // 4) * 8, 8)
    loads = []
    for src, dst in (
        (k_hbm.at[0], keys.at[pl.ds(OWN, ROWS)]),
        (v_hbm.at[0], vals.at[pl.ds(OWN, ROWS)]),
        (q_hbm.at[0], q_ref),
        (g_hbm.at[0], g_ref),
        (kinds_hbm.at[pl.ds(tile, 8)], kinds),
        (start_hbm.at[pl.ds(tile, 8)], starts),
    ):
        copy = pltpu.make_async_copy(src, dst, local_sem.at[len(loads)])
        copy.start()
        loads.append(copy)

    def remote(index, src, dst, peer):
        return pltpu.make_async_remote_copy(
            src_ref=src, dst_ref=dst, send_sem=send_sem.at[index],
            recv_sem=recv_sem.at[index], device_id=peer, device_id_type=MESH,
        )

    def rows(ref, first):
        return ref.at[pl.ds(first, ROWS)]

    loads[0].wait()
    loads[1].wait()
    pl.semaphore_wait(barrier, 3)

    near = [remote(i, rows(ref, OWN), rows(ref, BACK2), later) for i, ref in enumerate((keys, vals))]
    cross_even = [remote(2 + i, rows(ref, OWN), rows(ref, BACK1), across) for i, ref in enumerate((keys, vals))]
    cross_odd = [remote(2 + i, rows(ref, BACK2), rows(ref, BACK1), across) for i, ref in enumerate((keys, vals))]
    onward = [remote(4 + i, rows(ref, BACK1), rows(ref, BACK3), later) for i, ref in enumerate((keys, vals))]

    @pl.when(side == 0)
    def _():
        cross_even[0].start()

    near[0].start()
    near[1].start()

    @pl.when(side == 0)
    def _():
        cross_even[1].start()

    for i in range(2):
        near[i].wait_recv()

        @pl.when(side == 1)
        def _():
            cross_odd[i].start()

    for copy in loads[2:]:
        copy.wait()

    lane = lax.broadcasted_iota(jnp.int32, (1, BLK), 1)
    sub = lax.broadcasted_iota(jnp.int32, (BLK, BLK), 0)
    for b in range(2):
        at = lax.rem(owner, 4) * 2 + b
        kind_row = kinds[pl.ds(at, 1), :]
        start_row = starts[pl.ds(at, 1), :]
        block = owner * 2 + b
        token = block * BLK + lane
        for d in range(REACH + 1):
            kind = jnp.broadcast_to(kind_row[:, d : d + 1], (1, BLK))
            low = jnp.where(kind == 2, start_row, jnp.where(kind == 3, FAR, -FAR))
            high = jnp.where(kind == 0, FAR, token)
            pos = (block - d) * BLK + sub
            bias[b, pl.ds(block_row(b, d), BLK), :] = jnp.where(
                (pos >= low) & (pos <= high), 0.0, -1e30
            ).astype(jnp.float32)

    acc_k[...] = jnp.zeros_like(acc_k)
    acc_v[...] = jnp.zeros_like(acc_v)
    scale = HD ** -0.5
    scale2 = scale * LOG2E

    def stacked(ref, b, pair):
        both = ref[pl.ds(b * BLK, BLK), pl.ds(pl.multiple_of(pair * 256, 256), 256)]
        return jnp.concatenate([both[:, :HD], both[:, HD:]], axis=0)

    def fold(x, op):
        return op(x.reshape(BLK // 8, 8, 256), axis=0)

    def masked(b, first, queries):
        mask = bias[b, pl.ds(first, BLK), :]
        return nt(keys[pl.ds(first, BLK), :], queries) * scale2 + jnp.concatenate([mask, mask], axis=1)

    def transposed(first):
        at = pl.ds(first, ROWS)
        keys_t[:, at] = keys[at, :].astype(jnp.float32).T.astype(jnp.bfloat16)
        vals_t[:, at] = vals[at, :].astype(jnp.float32).T.astype(jnp.bfloat16)

    far_rows = [[block_row(b, d) for d in range(REACH + 1) if block_row(b, d) // ROWS in (BACK1 // ROWS, BACK3 // ROWS)] for b in range(2)]
    near_rows = [[block_row(b, d) for d in range(REACH + 1) if block_row(b, d) // ROWS in (BACK2 // ROWS, OWN // ROWS)] for b in range(2)]

    def each_unit(step):
        def body(pair, carry):
            for b in range(2):
                step(b, pair, b * PAIRS + pair)
            return carry

        lax.fori_loop(0, PAIRS, body, 0)

    def early(b, pair, unit):
        queries, grads = stacked(q_ref, b, pair), stacked(g_ref, b, pair)
        top = None
        for first in near_rows[b]:
            score = masked(b, first, queries)
            prob[unit, pl.ds(first, BLK), :] = score
            part = fold(score, jnp.max)
            top = part if top is None else jnp.maximum(top, part)
            pgrad[unit, pl.ds(first, BLK), :] = nt(vals[pl.ds(first, BLK), :], grads)
        top8[unit] = top

    each_unit(early)
    transposed(BACK2)
    transposed(OWN)

    def wait_cross(i):
        cross_even[i].wait_recv()
        onward[i].start()
        onward[i].wait_recv()

    wait_cross(0)

    def add_to(acc, b, wanted, half, unit, other):
        runs = []
        for first in sorted(wanted):
            if runs and runs[-1][1] == first:
                runs[-1][1] = first + BLK
            else:
                runs.append([first, first + BLK])
        for first, end in runs:
            at = pl.ds(first, end - first)
            acc[at, :] += nn(half[unit, at, :], other)

    def softmax(b, pair, unit):
        queries = stacked(q_ref, b, pair)
        top = top8[unit]
        for first in far_rows[b]:
            score = masked(b, first, queries)
            prob[unit, pl.ds(first, BLK), :] = score
            top = jnp.maximum(top, fold(score, jnp.max))
        top = jnp.max(top, axis=0, keepdims=True)
        total = jnp.zeros((8, 256), jnp.float32)
        for first in far_rows[b] + near_rows[b]:
            value = jnp.exp2(prob[unit, pl.ds(first, BLK), :] - top)
            prob[unit, pl.ds(first, BLK), :] = value
            total = total + fold(value, jnp.sum)
        share = 1.0 / jnp.sum(total, axis=0, keepdims=True)
        for first in far_rows[b] + near_rows[b]:
            value = prob[unit, pl.ds(first, BLK), :] * share
            prob[unit, pl.ds(first, BLK), :] = value
            prob_half[unit, pl.ds(first, BLK), :] = value.astype(jnp.bfloat16)
        add_to(acc_v, b, far_rows[b], prob_half, unit, stacked(g_ref, b, pair))

    each_unit(softmax)

    def copies(i):
        return (
            remote(6 + i, part3.at[i], got3.at[i], earlier),
            remote(8 + i, sum1.at[i], got1.at[i], earlier),
            remote(10 + i, got1.at[i], gotx.at[i], across),
            remote(10 + i, sum1.at[i], gotx.at[i], across),
            remote(12 + i, part2.at[i], got2.at[i], earlier),
        )

    home = [copies(0), copies(1)]

    def send_three(i, acc, factor):
        part3[i] = (acc[pl.ds(BACK3, ROWS), :] * factor).astype(jnp.bfloat16)
        home[i][0].start()

    def send_two(i, acc, factor):
        part2[i] = (acc[pl.ds(BACK2, ROWS), :] * factor).astype(jnp.bfloat16)
        home[i][4].start()

    def send_one(i, acc, factor):
        home[i][0].wait_recv()
        sum1[i] = (acc[pl.ds(BACK1, ROWS), :] * factor + got3[i].astype(jnp.float32)).astype(jnp.bfloat16)

        @pl.when(side == 0)
        def _():
            home[i][1].start()

        @pl.when(side == 1)
        def _():
            home[i][3].start()

    def send_across(i):
        @pl.when(side == 0)
        def _():
            home[i][1].wait_recv()
            home[i][2].start()

    send_three(0, acc_v, 1.0)

    def near_values(b, pair, unit):
        add_to(acc_v, b, near_rows[b], prob_half, unit, stacked(g_ref, b, pair))

    each_unit(near_values)
    send_one(0, acc_v, 1.0)
    send_two(0, acc_v, 1.0)
    send_across(0)

    wait_cross(1)

    def far_grads(b, pair, unit):
        queries, grads = stacked(q_ref, b, pair), stacked(g_ref, b, pair)
        dots = jnp.zeros((8, 256), jnp.float32)
        for first in near_rows[b]:
            at = pl.ds(first, BLK)
            dots = dots + fold(prob[unit, at, :] * pgrad[unit, at, :], jnp.sum)
        for first in far_rows[b]:
            at = pl.ds(first, BLK)
            value = nt(vals[at, :], grads)
            pgrad[unit, at, :] = value
            dots = dots + fold(prob[unit, at, :] * value, jnp.sum)
        dots = jnp.broadcast_to(jnp.sum(dots, axis=0, keepdims=True), (8, 256))
        dot8[unit] = dots
        for first in far_rows[b]:
            at = pl.ds(first, BLK)
            score_half[unit, at, :] = (
                prob[unit, at, :] * (pgrad[unit, at, :] - dots[:1])
            ).astype(jnp.bfloat16)
        add_to(acc_k, b, far_rows[b], score_half, unit, queries)

    each_unit(far_grads)
    send_three(1, acc_k, scale)

    def near_grads(b, pair, unit):
        dots = dot8[unit][:1]
        for first in near_rows[b]:
            at = pl.ds(first, BLK)
            score_half[unit, at, :] = (
                prob[unit, at, :] * (pgrad[unit, at, :] - dots)
            ).astype(jnp.bfloat16)
        add_to(acc_k, b, near_rows[b], score_half, unit, stacked(q_ref, b, pair))

    each_unit(near_grads)
    send_one(1, acc_k, scale)
    send_two(1, acc_k, scale)
    transposed(BACK1)
    transposed(BACK3)
    send_across(1)

    def outputs(b, pair, unit):
        window = pl.ds(block_row(b, REACH), (REACH + 1) * BLK)
        for ref, wide, half, factor in (
            (out_ref, vals_t, prob_half, None),
            (gq_ref, keys_t, score_half, scale),
        ):
            value = nn(wide[:, window], half[unit, window, :])
            if factor is not None:
                value = value * factor
            value = value.T.astype(jnp.bfloat16)
            for h in range(2):
                columns = pl.ds(pl.multiple_of(pair * 256 + h * HD, HD), HD)
                ref[pl.ds(b * BLK, BLK), columns] = value[h * BLK : (h + 1) * BLK, :]

    each_unit(outputs)
    stores = [
        pltpu.make_async_copy(out_ref, out_hbm.at[0], local_sem.at[6]),
        pltpu.make_async_copy(gq_ref, gq_hbm.at[0], local_sem.at[7]),
    ]
    for copy in stores:
        copy.start()

    for i, acc, factor, target in ((0, acc_v, 1.0, gv_hbm), (1, acc_k, scale, gk_hbm)):
        home[i][4].wait_recv()
        home[i][2].wait_recv()
        final[i] = (
            acc[pl.ds(OWN, ROWS), :] * factor
            + got2[i].astype(jnp.float32)
            + gotx[i].astype(jnp.float32)
        ).astype(jnp.bfloat16)
        copy = pltpu.make_async_copy(final.at[i], target.at[0], local_sem.at[8 + i])
        copy.start()
        stores.append(copy)

    for copy in near + cross_even + onward:
        copy.wait_send()
    for i in range(2):
        home[i][0].wait_send()
        home[i][2].wait_send()
        home[i][4].wait_send()

        @pl.when(side == 0)
        def _():
            home[i][1].wait_send()

    for copy in stores:
        copy.wait()


def local(query_states, key_states, value_states, grad_output, pair_kinds, row_start):
    half, full = jnp.bfloat16, jnp.float32
    window = 4 * ROWS
    units = 2 * PAIRS
    moved = pltpu.VMEM((2, ROWS, HD), half)
    hbm = pl.BlockSpec(memory_space=pl.ANY)
    return pl.pallas_call(
        kernel,
        out_shape=tuple(
            jax.ShapeDtypeStruct(x.shape, half)
            for x in (query_states, query_states, key_states, key_states)
        ),
        in_specs=[hbm] * 6,
        out_specs=(hbm,) * 4,
        scratch_shapes=[
            pltpu.VMEM((ROWS, GQ * HD), half),
            pltpu.VMEM((ROWS, GQ * HD), half),
            pltpu.VMEM((window, HD), half),
            pltpu.VMEM((window, HD), half),
            pltpu.VMEM((HD, window), half),
            pltpu.VMEM((HD, window), half),
            pltpu.VMEM((2, window, BLK), full),
            pltpu.VMEM((8, REACH + 1), jnp.int32),
            pltpu.VMEM((8, BLK), jnp.int32),
            pltpu.VMEM((units, window, 256), full),
            pltpu.VMEM((units, window, 256), full),
            pltpu.VMEM((units, window, 256), half),
            pltpu.VMEM((units, window, 256), half),
            pltpu.VMEM((units, 8, 256), full),
            pltpu.VMEM((units, 8, 256), full),
            pltpu.VMEM((window, HD), full),
            pltpu.VMEM((window, HD), full),
            moved, moved, moved, moved, moved, moved, moved,
            pltpu.VMEM((ROWS, GQ * HD), half),
            pltpu.VMEM((ROWS, GQ * HD), half),
            moved,
            pltpu.SemaphoreType.DMA((10,)),
            pltpu.SemaphoreType.DMA((14,)),
            pltpu.SemaphoreType.DMA((14,)),
        ],
        compiler_params=pltpu.CompilerParams(
            collective_id=0, has_side_effects=True, vmem_limit_bytes=56 << 20
        ),
        name="exchange",
    )(query_states, key_states, value_states, grad_output, pair_kinds, row_start.reshape(-1, BLK))


def solution(mesh):
    split = P(("grp", "cp"), None, None)
    return jax.shard_map(
        local,
        mesh=mesh,
        in_specs=(split, split, split, split, P(), P()),
        out_specs=(split, split, split, split),
        check_vma=False,
    )
```
